32 devices in a mesh: dp: 4 (over x, core), mp: 8 (over z, y).
Axes of the slice: x: 2, y: 2, z: 4, core: 2. Of those that a mesh axis runs over, the one named last changes fastest.
Arguments:
- gradients: bfloat16 [4, 4096, 4096], P('dp', None, 'mp'), may hold values from -40 to 40
- owner_table: int32 [128], replicated, may hold values from 0 to 7, as said below
Outputs:
- root_stacks: float32 [8, 24, 512, 512], P('mp', 'dp')
- slab_roots: float32 [16, 512, 4096], P(None, 'dp', 'mp')
The draws below stay inside these ranges and needn't reach their ends.
Inputs may be any that keep to these rules, and one draw needn't show every extreme that they name: `owner_table`: statistic m * 16 + i belongs to column slab m. No owner is named by more than 24 statistics and some owner by exactly 24; among the 16 statistics of one column slab no owner is named more than 3 times, and some slab names some owner exactly 3 times.
All inputs are finite; a program needn't handle non-finite values.
Results may differ from the reference program's by a relative error of at most 0.0017.
Values may be sent and summed in bfloat16 or wider, within the bound.
A program may use at most 320 MiB of HBM per device.

```python
import jax
import jax.numpy as jnp
from jax import lax

BLOCK = 512
ROWS = 4096
ITERS = 3
CAP = 24
COLS = 4096
ROW_BLOCKS = 8
PER_SLAB = 16
STATS = 128
N_DP = 4
N_MP = 8


def draw_gradients(key, part):
    noise_key = jax.random.fold_in(key, 0)
    shape_full = (N_DP, ROWS, COLS)
    values = jax.random.normal(noise_key, shape_full, jnp.float32)
    shard_scale = 1.0 + 2.0 * jnp.arange(N_DP, dtype=jnp.float32) / max(N_DP - 1, 1)
    values = values * shard_scale[:, None, None] * BLOCK ** (-0.5)
    return values.astype(jnp.bfloat16)


def draw_owner_table(key, part):
    per_slab_count = 2 * (ROWS // BLOCK)
    order_key, amount_key = jax.random.split(key)
    owner_order = jax.random.permutation(order_key, N_MP)
    half_count = N_MP // 2
    amount = jax.random.randint(amount_key, (half_count,), 0, CAP - per_slab_count + 1)
    amount = amount.at[0].set(CAP - per_slab_count)
    ranked = (per_slab_count + jnp.concatenate([amount, -amount])).astype(jnp.int32)
    owner_loads = jnp.zeros((N_MP,), jnp.int32).at[owner_order].set(ranked)
    load_ends = jnp.cumsum(owner_loads)
    positions = jnp.arange(N_MP * per_slab_count, dtype=jnp.int32)
    sorted_owner = jnp.sum((positions[:, None] >= load_ends[None, :]).astype(jnp.int32), axis=1)
    slab_index = positions // per_slab_count
    within_slab = positions % per_slab_count
    return sorted_owner[within_slab * N_MP + slab_index].astype(jnp.int32)


def setup_inputs(seed: int = 0) -> dict:
    keys = jax.random.split(jax.random.key(seed), 3)
    gradients = draw_gradients(jax.random.fold_in(keys[2], 71), 0)
    owner_table = draw_owner_table(jax.random.fold_in(keys[2], 71), 0)
    return dict(gradients=gradients, owner_table=owner_table)


def batched(first, second):
    return jnp.einsum('kab,kbc->kac', first, second, precision=lax.Precision.HIGHEST)

def newton_roots(statistics, iterations):
    matrix_size = statistics.shape[-1]
    identity = jnp.eye(matrix_size, dtype=jnp.float32)
    diagonal_mean = lax.optimization_barrier(jnp.mean(jnp.diagonal(statistics, axis1=1, axis2=2), axis=1))
    damped = statistics + 0.1 * diagonal_mean[:, None, None] * identity[None]
    mean_square = lax.optimization_barrier(jnp.mean(damped * damped, axis=(1, 2)))
    norm_scale = matrix_size * jnp.sqrt(mean_square + 1e-06)
    matrix = damped / norm_scale[:, None, None]
    root_scale = norm_scale ** (-0.25)
    current = matrix
    for iteration in range(iterations):
        factor = (5.0 * identity - matrix) * 0.25
        if iteration == 0:
            current = factor * root_scale[:, None, None]
        else:
            current = batched(current, factor)
        if iteration + 1 < iterations:
            square = batched(factor, factor)
            matrix = batched(square, batched(square, matrix))
    return current

def reference(gradients, owner_table):

    def slab_work(column):
        first_column = (column * BLOCK).astype(jnp.int32)
        column_slab = lax.dynamic_slice_in_dim(gradients, first_column, BLOCK, 2).astype(jnp.float32)
        blocks = column_slab.reshape(N_DP, ROW_BLOCKS, BLOCK, BLOCK)
        left_gram = jnp.einsum('drab,drcb->drac', blocks, blocks)
        right_gram = jnp.einsum('drab,drac->drbc', blocks, blocks)
        partial_value = jnp.stack([left_gram, right_gram], axis=2).reshape(N_DP, PER_SLAB, BLOCK, BLOCK)
        rounded = lax.optimization_barrier(partial_value.astype(jnp.bfloat16)).astype(jnp.float32)
        statistics = lax.optimization_barrier(jnp.sum(rounded, axis=0)) * (1.0 / N_DP)
        return newton_roots(statistics, ITERS)
    all_roots = lax.map(slab_work, jnp.arange(N_MP, dtype=jnp.int32))
    slab_roots = jnp.transpose(all_roots, (1, 2, 0, 3)).reshape(PER_SLAB, BLOCK, COLS)
    owner_ids = jnp.arange(N_MP, dtype=jnp.int32)
    onehot = (owner_table[:, None] == owner_ids[None, :]).astype(jnp.int32)
    slot_number = lax.optimization_barrier(jnp.sum((jnp.cumsum(onehot, axis=0) - onehot) * onehot, axis=1)).astype(jnp.int32)
    flat_roots = all_roots.reshape(STATS, BLOCK, BLOCK)
    root_stacks = jnp.zeros((N_MP, CAP, BLOCK, BLOCK), jnp.float32).at[owner_table, slot_number].set(flat_roots)
    return (root_stacks, slab_roots)
```

```python
import jax
import jax.numpy as jnp
from jax import lax
from jax.experimental import pallas as pl
from jax.experimental.pallas import tpu as pltpu
from jax.sharding import PartitionSpec as P

ITERS = 3
CAP = 24


def batched(first, second):
    return jnp.einsum("kab,kbc->kac", first, second, precision=lax.Precision.HIGHEST)


def newton_roots(statistics, iterations):
    matrix_size = statistics.shape[-1]
    identity = jnp.eye(matrix_size, dtype=jnp.float32)
    diagonal_mean = jnp.mean(jnp.diagonal(statistics, axis1=1, axis2=2), axis=1)
    damped = statistics + 0.1 * diagonal_mean[:, None, None] * identity[None]
    mean_square = jnp.mean(damped * damped, axis=(1, 2))
    norm_scale = matrix_size * jnp.sqrt(mean_square + 1e-06)
    matrix = damped / norm_scale[:, None, None]
    root_scale = norm_scale ** (-0.25)
    current = matrix
    for iteration in range(iterations):
        factor = (5.0 * identity - matrix) * 0.25
        if iteration == 0:
            current = factor * root_scale[:, None, None]
        else:
            current = batched(current, factor)
        if iteration + 1 < iterations:
            square = batched(factor, factor)
            matrix = batched(square, batched(square, matrix))
    return current


def pick_rows(source, match_table):
    labels = jnp.arange(match_table.shape[1], dtype=jnp.int32)
    pick_index = jnp.sum(match_table * labels[None, :], axis=1)
    is_valid = jnp.sum(match_table, axis=1).astype(jnp.float32)
    return jnp.take(source, pick_index, axis=0) * is_valid[:, None, None]


def make_plan(owner_table, model_index, model_count, per_slab, pair_count):
    stat_count = owner_table.shape[0]
    owner_ids = jnp.arange(model_count, dtype=jnp.int32)
    onehot = (owner_table[:, None] == owner_ids[None, :]).astype(jnp.int32)
    slot_number = jnp.sum((jnp.cumsum(onehot, axis=0) - onehot) * onehot, axis=1)
    owner_grid = onehot.reshape(model_count, per_slab, model_count)
    pair_rank = jnp.sum((jnp.cumsum(owner_grid, axis=1) - owner_grid) * owner_grid, axis=2).reshape(
        stat_count
    )
    stat_ids = jnp.arange(stat_count, dtype=jnp.int32)
    position = stat_ids // per_slab * pair_count + pair_rank
    owner_loads = jnp.sum(onehot, axis=0)
    first_stat = model_index * per_slab
    targets = lax.dynamic_slice_in_dim(owner_table * pair_count + pair_rank, first_stat, per_slab)
    slot_ids = jnp.arange(CAP, dtype=jnp.int32)
    slot_match = (
        (owner_table[None, :] == model_index) & (slot_number[None, :] == slot_ids[:, None])
    ).astype(jnp.int32)
    stack_index = jnp.sum(slot_match * position[None, :], axis=1)
    stack_valid = jnp.sum(slot_match, axis=1)
    return (targets, stack_index, stack_valid, owner_loads)


def to_owner(pieces, route_plan, model_count, pair_count):
    targets, stack_index, stack_valid, owner_loads = route_plan
    places = jnp.arange(model_count * pair_count, dtype=jnp.int32)
    send_match = (places[:, None] == targets[None, :]).astype(jnp.int32)
    incoming = lax.all_to_all(
        pick_rows(pieces, send_match), "mp", split_axis=0, concat_axis=0, tiled=True
    )
    slot_match = (stack_index[:, None] == places[None, :]).astype(jnp.int32) * stack_valid[:, None]
    slot_stack = pick_rows(incoming, slot_match)
    return lax.all_to_all(slot_stack, "dp", split_axis=0, concat_axis=1, tiled=True)


def row_sums(rounded, data_count):
    return lax.psum_scatter(
        rounded.astype(jnp.bfloat16), "dp", scatter_dimension=1, tiled=True
    ).astype(jnp.float32) * (1.0 / data_count)


def on_device(gradients, owner_table):
    data_count = lax.axis_size("dp")
    model_count = lax.axis_size("mp")
    model_index = lax.axis_index("mp")
    block_size = gradients.shape[2]
    row_blocks = gradients.shape[1] // block_size
    per_slab = 2 * row_blocks
    pair_count = (CAP + model_count - 1) // model_count
    local_blocks = gradients[0].reshape(row_blocks, block_size, block_size)
    left_gram = jnp.einsum(
        "rab,rcb->rac", local_blocks, local_blocks, preferred_element_type=jnp.float32
    )
    right_gram = jnp.einsum(
        "rab,rac->rbc", local_blocks, local_blocks, preferred_element_type=jnp.float32
    )
    partial_value = jnp.stack([left_gram, right_gram], axis=1).reshape(
        per_slab, block_size, block_size
    )
    rounded = lax.optimization_barrier(partial_value.astype(jnp.bfloat16)).astype(jnp.float32)
    route_plan = make_plan(owner_table, model_index, model_count, per_slab, pair_count)
    stat_sums = row_sums(rounded, data_count)
    whole_stats = lax.all_to_all(stat_sums, "dp", split_axis=0, concat_axis=1, tiled=True)
    home_roots = newton_roots(whole_stats, ITERS)
    slab_roots = lax.all_to_all(home_roots, "dp", split_axis=1, concat_axis=0, tiled=True)
    root_stacks = to_owner(slab_roots, route_plan, model_count, pair_count)
    return (root_stacks[None], slab_roots)


def iota2(shape, axis):
    return lax.broadcasted_iota(jnp.int32, shape, axis)


def matmul(first, second):
    return jnp.dot(
        first.astype(jnp.bfloat16), second.astype(jnp.bfloat16), preferred_element_type=jnp.float32
    )


def fold_upper(store, full):
    store(0, 128, 0, 512, full[0:128, :])
    store(128, 256, 128, 512, full[128:256, 128:512])
    store(128, 256, 0, 128, full[384:512, 384:512])
    store(256, 320, 0, 256, full[256:320, 256:512])
    store(256, 320, 256, 512, full[320:384, 256:512])


def gram_kernel(where_ref, grad_ref, out_ref):
    block = grad_ref[0]
    for kind in range(2):
        flipped = block.T
        full = jnp.dot(block, flipped, preferred_element_type=jnp.float32) if kind == 0 else jnp.dot(
            flipped, block, preferred_element_type=jnp.float32
        )
        full = full.astype(jnp.bfloat16)

        def store(r0, r1, c0, c1, value, kind=kind):
            out_ref[0, kind, r0:r1, c0:c1] = value

        fold_upper(store, full)


def grams(where, gradients, relative_core):
    size = gradients.shape[2]

    def grad_map(step, where_ref):
        target = where_ref[0] ^ relative_core ^ ((1 - step // 2) * 2)
        return (0, target * 2 + step % 2, 0)

    return pl.pallas_call(
        gram_kernel,
        grid_spec=pltpu.PrefetchScalarGridSpec(
            num_scalar_prefetch=1,
            grid=(4,),
            in_specs=[pl.BlockSpec((1, size, size), grad_map)],
            out_specs=pl.BlockSpec((1, 2, 320, size), lambda step, where_ref: (step, 0, 0, 0)),
        ),
        out_shape=jax.ShapeDtypeStruct((4, 2, 320, size), jnp.bfloat16),
        cost_estimate=pl.CostEstimate(flops=8 * 2 * size**3, bytes_accessed=5 * 2**20, transcendentals=0),
        name="grams_%d" % relative_core,
    )(where, gradients)


def unfold(source, whole):
    whole[0:128, :] = source(0, 128, 0, 512)
    whole[128:256, 128:512] = source(128, 256, 128, 512)
    whole[384:512, 384:512] = source(128, 256, 0, 128)
    whole[256:320, 256:512] = source(256, 320, 0, 256)
    whole[320:384, 256:512] = source(256, 320, 256, 512)
    for i in range(4):
        for j in range(i + 1, 4):
            whole[j * 128 : j * 128 + 128, i * 128 : i * 128 + 128] = whole[
                i * 128 : i * 128 + 128, j * 128 : j * 128 + 128
            ].T


def newton_kernel(where_ref, own_ref, core_ref, far_ref, *rest):
    outs, whole = rest[:4], rest[4]
    size = whole.shape[0]

    def source(r0, r1, c0, c1):
        return (
            own_ref[0, r0:r1, c0:c1].astype(jnp.float32)
            + core_ref[0, r0:r1, c0:c1].astype(jnp.float32)
            + far_ref[0, r0:r1, c0:c1].astype(jnp.float32)
        ) * 0.25

    unfold(source, whole)
    identity = (iota2((size, size), 0) == iota2((size, size), 1)).astype(jnp.float32)
    statistic = whole[...]
    diagonal = jnp.sum(jnp.sum(statistic * identity, axis=0, keepdims=True), axis=1, keepdims=True) / size
    damped = statistic + 0.1 * diagonal * identity
    square = jnp.sum(jnp.sum(damped * damped, axis=0, keepdims=True), axis=1, keepdims=True) / (size * size)
    norm_scale = size * jnp.sqrt(square + 1e-06)
    root_scale = 1.0 / jnp.sqrt(jnp.sqrt(norm_scale))
    first = damped * (1.0 / norm_scale)

    def advance(matrix):
        part = matmul(matrix, matrix) * 0.0625 - 0.625 * matrix
        half = 1.5625 * matrix + matmul(part, matrix)
        return 1.5625 * half + matmul(part, half)

    second = advance(first)
    product = matmul(first, second) * 0.0625 - 0.3125 * (first + second)
    third = advance(second)
    rest_part = 1.25 * product - 0.390625 * third - 0.25 * matmul(product, third)
    whole[...] = rest_part * root_scale
    centre = root_scale * 1.953125
    high = centre.astype(jnp.bfloat16).astype(jnp.float32)
    low = centre - high
    for relative in range(4):
        target = where_ref[0] ^ relative
        rows = pl.multiple_of(target * 128, 128)
        outs[relative][0] = whole[pl.ds(rows, 128), :].astype(jnp.bfloat16)
        last = whole[pl.ds(rows + 112, 16), pl.ds(rows, 128)]
        row, lane = iota2((16, 128), 0), iota2((16, 128), 1)
        last = jnp.where((row == 15) & (lane == 0), high, last)
        last = jnp.where((row == 15) & (lane == 1), low, last)
        outs[relative][0, 112:128, pl.ds(rows, 128)] = last.astype(jnp.bfloat16)


def newton(where, own, core, far, chunk):
    size = own.shape[-1]
    folded = own.shape[-2]
    flat = lambda array: array.reshape(-1, folded, size)
    spec = lambda offset: pl.BlockSpec((1, folded, size), lambda step, where_ref: (offset + step, 0, 0))
    return pl.pallas_call(
        newton_kernel,
        grid_spec=pltpu.PrefetchScalarGridSpec(
            num_scalar_prefetch=1,
            grid=(2,),
            in_specs=[spec(4 + chunk * 2), spec(4 + chunk * 2), spec(0)],
            out_specs=[pl.BlockSpec((1, 128, size), lambda step, where_ref: (step, 0, 0))] * 4,
            scratch_shapes=[pltpu.VMEM((size, size), jnp.float32)],
        ),
        out_shape=[jax.ShapeDtypeStruct((2, 128, size), jnp.bfloat16)] * 4,
        cost_estimate=pl.CostEstimate(flops=16 * 2 * size**3, bytes_accessed=4 * 2**20, transcendentals=0),
        name="newton_%d" % chunk,
    )(where, flat(own), flat(core), flat(far))


def opened(tile):
    row, lane = iota2((128, 128), 0), iota2((128, 128), 1)
    line = iota2((1, 128), 1)
    last = tile[127:128, :]
    pick = lambda values, mask: jnp.sum(jnp.where(mask, values, 0.0), axis=1, keepdims=True)
    centre = pick(last, line < 2)
    first_value = pick(tile[0:1, :], line == 127)
    second_value = pick(tile[1:2, :], line == 127)
    tile = jnp.where((row == 127) & (lane == 0), first_value, tile)
    tile = jnp.where((row == 127) & (lane == 1), second_value, tile)
    return tile + jnp.where(row == lane, centre, 0.0)


def locate(stat, device):
    return (stat // 4) ^ device, (stat % 4) // 2, stat % 2


def gather_rows(where, refs, held):
    for chunk in range(2):
        for relative in range(4):
            for place in range(2):
                target = (where ^ relative) * 4 + chunk * 2 + place
                held[target] = refs[chunk * 4 + relative][place]


def slab_kernel(where_ref, *rest):
    refs, out_ref = rest[:8], rest[8]
    device = where_ref[0]
    columns = pl.multiple_of(device * 128, 128)
    for chunk in range(2):
        for relative in range(4):
            base = (device ^ relative) * 4 + chunk * 2

            def body(place, carry):
                value = refs[chunk * 4 + relative][place].astype(jnp.float32)
                out_ref[base + place] = value
                tile = refs[chunk * 4 + relative][place, :, pl.ds(columns, 128)].astype(jnp.float32)
                out_ref[base + place, :, pl.ds(columns, 128)] = opened(tile)
                return carry

            lax.fori_loop(0, 2, body, 0)


def slab_rows(where, pieces, stats):
    size = pieces[0].shape[-1]
    return pl.pallas_call(
        slab_kernel,
        in_specs=[pl.BlockSpec(memory_space=pltpu.SMEM)] + [pl.BlockSpec(memory_space=pltpu.VMEM)] * 8,
        out_specs=pl.BlockSpec(memory_space=pltpu.VMEM),
        out_shape=jax.ShapeDtypeStruct((stats, 128, size), jnp.float32),
        cost_estimate=pl.CostEstimate(flops=2**22, bytes_accessed=6 * 2**20, transcendentals=0),
        name="slab_rows",
    )(where, *pieces)


def send_kernel(where_ref, index_ref, valid_ref, *rest):
    refs, out_ref, held, tiles = rest[:8], rest[8], rest[9], rest[10]
    device = where_ref[0]
    gather_rows(device, refs, held)
    own = pl.multiple_of(device * 128, 128)
    after = pl.multiple_of(((device + 1) % 4) * 128, 128)
    across = pl.multiple_of((device ^ 2) * 128, 128)

    def body(place, carry):
        @pl.when(valid_ref[place] > 0)
        def _():
            stat = index_ref[place]
            out_ref[place, 0:128, 0:128] = held[stat, :, pl.ds(own, 128)]
            out_ref[place, 0:128, 128:256] = held[stat, :, pl.ds(after, 128)]
            tile = held[stat, :, pl.ds(across, 128)].astype(jnp.float32)
            half = jnp.where(device < 2, tile[0:64, :], tile.T[64:128, :]).astype(jnp.bfloat16)
            out_ref[place, 128:160, 0:128] = half[0:32, :]
            out_ref[place, 128:160, 128:256] = half[32:64, :]

        @pl.when(valid_ref[place] == 0)
        def _():
            out_ref[place] = jnp.zeros(out_ref.shape[1:], out_ref.dtype)

        return carry

    lax.fori_loop(0, out_ref.shape[0], body, 0)


def send_rows(where, index, valid, pieces, stats):
    size = pieces[0].shape[-1]
    places = index.shape[0]
    smem = pl.BlockSpec(memory_space=pltpu.SMEM)
    return pl.pallas_call(
        send_kernel,
        in_specs=[smem] * 3 + [pl.BlockSpec(memory_space=pltpu.VMEM)] * 8,
        out_specs=pl.BlockSpec(memory_space=pltpu.VMEM),
        out_shape=jax.ShapeDtypeStruct((places, 160, 256), jnp.bfloat16),
        scratch_shapes=[
            pltpu.VMEM((stats, 128, size), jnp.bfloat16),
            pltpu.VMEM((128, 128), jnp.float32),
        ],
        cost_estimate=pl.CostEstimate(flops=2**22, bytes_accessed=4 * 2**20, transcendentals=0),
        name="send_rows",
    )(where, index, valid, *pieces)


def slot_kernel(index_ref, valid_ref, source_ref, out_ref):
    def body(slot, carry):
        @pl.when(valid_ref[slot] > 0)
        def _():
            out_ref[slot] = source_ref[index_ref[slot]]

        @pl.when(valid_ref[slot] == 0)
        def _():
            out_ref[slot] = jnp.zeros(out_ref.shape[1:], out_ref.dtype)

        return carry

    lax.fori_loop(0, out_ref.shape[0], body, 0)


def slot_rows(index, valid, source):
    smem = pl.BlockSpec(memory_space=pltpu.SMEM)
    return pl.pallas_call(
        slot_kernel,
        in_specs=[smem, smem, pl.BlockSpec(memory_space=pltpu.VMEM)],
        out_specs=pl.BlockSpec(memory_space=pltpu.VMEM),
        out_shape=jax.ShapeDtypeStruct((index.shape[0],) + source.shape[1:], source.dtype),
        cost_estimate=pl.CostEstimate(flops=2**20, bytes_accessed=4 * 2**20, transcendentals=0),
        name="slot_rows",
    )(index, valid, source)


def stack_kernel(piece_ref, out_ref):
    tile_at = lambda i: slice(i * 128, i * 128 + 128)
    for i in range(4):
        out_ref[0, tile_at(i), tile_at(i)] = opened(piece_ref[i, 0, 0:128, 0:128].astype(jnp.float32))
        j = (i + 1) % 4
        tile = piece_ref[i, 0, 0:128, 128:256].astype(jnp.float32)
        out_ref[0, tile_at(i), tile_at(j)] = tile
        out_ref[0, tile_at(j), tile_at(i)] = tile.T
    for i in range(2):
        parts = []
        for source in (i, i + 2):
            parts += [piece_ref[source, 0, 128:160, 0:128], piece_ref[source, 0, 128:160, 128:256]]
        tile = jnp.concatenate([part.astype(jnp.float32) for part in parts], axis=0)
        out_ref[0, tile_at(i), tile_at(i + 2)] = tile
        out_ref[0, tile_at(i + 2), tile_at(i)] = tile.T


def stack_rows(pieces, size):
    slots = pieces.shape[1]
    return pl.pallas_call(
        stack_kernel,
        grid=(slots,),
        in_specs=[pl.BlockSpec((4, 1, 160, 256), lambda slot: (0, slot, 0, 0))],
        out_specs=pl.BlockSpec((1, size, size), lambda slot: (slot, 0, 0)),
        out_shape=jax.ShapeDtypeStruct((slots, size, size), jnp.float32),
        cost_estimate=pl.CostEstimate(flops=2**22, bytes_accessed=8 * 2**20, transcendentals=0),
        name="stack_rows",
    )(pieces)


def exchange(array, relative):
    return lax.ppermute(array, "dp", [(i, i ^ relative) for i in range(4)])


def on_quad(gradients, owner_table):
    model_count = lax.axis_size("mp")
    model_index = lax.axis_index("mp")
    device = lax.axis_index("dp")
    where = device.astype(jnp.int32).reshape(1)
    size = gradients.shape[2]
    per_slab = 2 * (gradients.shape[1] // size)
    pair_count = (CAP + model_count - 1) // model_count
    targets, stack_index, stack_valid, _ = make_plan(
        owner_table, model_index, model_count, per_slab, pair_count
    )
    places = jnp.arange(model_count * pair_count, dtype=jnp.int32)
    send_match = (places[:, None] == targets[None, :]).astype(jnp.int32)
    send_index = jnp.sum(send_match * jnp.arange(per_slab, dtype=jnp.int32)[None, :], axis=1)
    send_valid = jnp.sum(send_match, axis=1)

    received = exchange(grams(where, gradients, 1), 1)
    own = grams(where, gradients, 0)
    pieces = []
    for chunk in range(2):
        summed = (own[chunk].astype(jnp.float32) + received[chunk].astype(jnp.float32)).astype(jnp.bfloat16)
        far = exchange(summed, 2)
        roots = newton(where, own, received, far, chunk)
        pieces += [roots[0]] + [exchange(roots[relative], relative) for relative in (1, 2, 3)]
    sent = send_rows(where, send_index, send_valid, pieces, per_slab)
    incoming = lax.all_to_all(sent, "mp", split_axis=0, concat_axis=0, tiled=True)
    slab = slab_rows(where, pieces, per_slab)
    slots = slot_rows(stack_index, stack_valid, incoming)
    shared = lax.all_to_all(slots, "dp", split_axis=0, concat_axis=0, tiled=True)
    stacks = stack_rows(shared.reshape(4, CAP // 4, 160, 256), size)
    return (stacks[None], slab)


def solution(mesh):
    placed = (P("dp", None, "mp"), P())

    def body(gradients, owner_table):
        size = gradients.shape[2]
        row_blocks = gradients.shape[1] // size
        if lax.axis_size("dp") == 4 and size == 512 and row_blocks == 8:
            return on_quad(gradients, owner_table)
        return on_device(gradients, owner_table)

    return jax.shard_map(
        body,
        mesh=mesh,
        in_specs=placed,
        out_specs=(P("mp", "dp", None, None), P(None, "dp", "mp")),
        check_vma=False,
    )
```

```python
import functools

import jax
import jax.numpy as jnp
from jax import lax
from jax.experimental import pallas as pl
from jax.experimental.pallas import tpu as pltpu
from jax.sharding import PartitionSpec as P

ITERS = 3
CAP = 24
PARTS = 5
MESH = pl.DeviceIdType.MESH


def batched(first, second):
    return jnp.einsum("kab,kbc->kac", first, second, precision=lax.Precision.HIGHEST)


def newton_roots(statistics, iterations):
    matrix_size = statistics.shape[-1]
    identity = jnp.eye(matrix_size, dtype=jnp.float32)
    diagonal_mean = jnp.mean(jnp.diagonal(statistics, axis1=1, axis2=2), axis=1)
    damped = statistics + 0.1 * diagonal_mean[:, None, None] * identity[None]
    mean_square = jnp.mean(damped * damped, axis=(1, 2))
    norm_scale = matrix_size * jnp.sqrt(mean_square + 1e-06)
    matrix = damped / norm_scale[:, None, None]
    root_scale = norm_scale ** (-0.25)
    current = matrix
    for iteration in range(iterations):
        factor = (5.0 * identity - matrix) * 0.25
        if iteration == 0:
            current = factor * root_scale[:, None, None]
        else:
            current = batched(current, factor)
        if iteration + 1 < iterations:
            square = batched(factor, factor)
            matrix = batched(square, batched(square, matrix))
    return current


def pick_rows(source, match_table):
    labels = jnp.arange(match_table.shape[1], dtype=jnp.int32)
    pick_index = jnp.sum(match_table * labels[None, :], axis=1)
    is_valid = jnp.sum(match_table, axis=1).astype(jnp.float32)
    return jnp.take(source, pick_index, axis=0) * is_valid[:, None, None]


def make_plan(owner_table, model_index, model_count, per_slab, pair_count):
    stat_count = owner_table.shape[0]
    owner_ids = jnp.arange(model_count, dtype=jnp.int32)
    onehot = (owner_table[:, None] == owner_ids[None, :]).astype(jnp.int32)
    slot_number = jnp.sum((jnp.cumsum(onehot, axis=0) - onehot) * onehot, axis=1)
    owner_grid = onehot.reshape(model_count, per_slab, model_count)
    pair_rank = jnp.sum((jnp.cumsum(owner_grid, axis=1) - owner_grid) * owner_grid, axis=2).reshape(
        stat_count
    )
    stat_ids = jnp.arange(stat_count, dtype=jnp.int32)
    position = stat_ids // per_slab * pair_count + pair_rank
    owner_loads = jnp.sum(onehot, axis=0)
    first_stat = model_index * per_slab
    targets = lax.dynamic_slice_in_dim(owner_table * pair_count + pair_rank, first_stat, per_slab)
    slot_ids = jnp.arange(CAP, dtype=jnp.int32)
    slot_match = (
        (owner_table[None, :] == model_index) & (slot_number[None, :] == slot_ids[:, None])
    ).astype(jnp.int32)
    stack_index = jnp.sum(slot_match * position[None, :], axis=1)
    stack_valid = jnp.sum(slot_match, axis=1)
    return (targets, stack_index, stack_valid, owner_loads)


def to_owner(pieces, route_plan, model_count, pair_count):
    targets, stack_index, stack_valid, owner_loads = route_plan
    places = jnp.arange(model_count * pair_count, dtype=jnp.int32)
    send_match = (places[:, None] == targets[None, :]).astype(jnp.int32)
    incoming = lax.all_to_all(
        pick_rows(pieces, send_match), "mp", split_axis=0, concat_axis=0, tiled=True
    )
    slot_match = (stack_index[:, None] == places[None, :]).astype(jnp.int32) * stack_valid[:, None]
    slot_stack = pick_rows(incoming, slot_match)
    return lax.all_to_all(slot_stack, "dp", split_axis=0, concat_axis=1, tiled=True)


def row_sums(rounded, data_count):
    return lax.psum_scatter(
        rounded.astype(jnp.bfloat16), "dp", scatter_dimension=1, tiled=True
    ).astype(jnp.float32) * (1.0 / data_count)


def on_device(gradients, owner_table):
    data_count = lax.axis_size("dp")
    model_count = lax.axis_size("mp")
    model_index = lax.axis_index("mp")
    block_size = gradients.shape[2]
    row_blocks = gradients.shape[1] // block_size
    per_slab = 2 * row_blocks
    pair_count = (CAP + model_count - 1) // model_count
    local_blocks = gradients[0].reshape(row_blocks, block_size, block_size)
    left_gram = jnp.einsum(
        "rab,rcb->rac", local_blocks, local_blocks, preferred_element_type=jnp.float32
    )
    right_gram = jnp.einsum(
        "rab,rac->rbc", local_blocks, local_blocks, preferred_element_type=jnp.float32
    )
    partial_value = jnp.stack([left_gram, right_gram], axis=1).reshape(
        per_slab, block_size, block_size
    )
    rounded = lax.optimization_barrier(partial_value.astype(jnp.bfloat16)).astype(jnp.float32)
    route_plan = make_plan(owner_table, model_index, model_count, per_slab, pair_count)
    stat_sums = row_sums(rounded, data_count)
    whole_stats = lax.all_to_all(stat_sums, "dp", split_axis=0, concat_axis=1, tiled=True)
    home_roots = newton_roots(whole_stats, ITERS)
    slab_roots = lax.all_to_all(home_roots, "dp", split_axis=1, concat_axis=0, tiled=True)
    root_stacks = to_owner(slab_roots, route_plan, model_count, pair_count)
    return (root_stacks[None], slab_roots)


def iota2(shape, axis):
    return lax.broadcasted_iota(jnp.int32, shape, axis)


def matmul(first, second):
    return jnp.dot(
        first.astype(jnp.bfloat16), second.astype(jnp.bfloat16), preferred_element_type=jnp.float32
    )


def fold_upper(store, full):
    store(0, 128, 0, 512, full[0:128, :])
    store(128, 256, 128, 512, full[128:256, 128:512])
    store(128, 256, 0, 128, full[384:512, 384:512])
    store(256, 320, 0, 256, full[256:320, 256:512])
    store(256, 320, 256, 512, full[320:384, 256:512])


def gram_kernel(where_ref, grad_ref, out_ref):
    block = grad_ref[0]
    for kind in range(2):
        flipped = block.T
        full = jnp.dot(block, flipped, preferred_element_type=jnp.float32) if kind == 0 else jnp.dot(
            flipped, block, preferred_element_type=jnp.float32
        )
        full = full.astype(jnp.bfloat16)

        def store(r0, r1, c0, c1, value, kind=kind):
            out_ref[0, kind, r0:r1, c0:c1] = value

        fold_upper(store, full)


def grams(where, gradients, relative_core):
    size = gradients.shape[2]

    def grad_map(step, where_ref):
        target = where_ref[0] ^ relative_core ^ ((1 - step // 2) * 2)
        return (0, target * 2 + step % 2, 0)

    return pl.pallas_call(
        gram_kernel,
        grid_spec=pltpu.PrefetchScalarGridSpec(
            num_scalar_prefetch=1,
            grid=(4,),
            in_specs=[pl.BlockSpec((1, size, size), grad_map)],
            out_specs=pl.BlockSpec((1, 2, 320, size), lambda step, where_ref: (step, 0, 0, 0)),
        ),
        out_shape=jax.ShapeDtypeStruct((4, 2, 320, size), jnp.bfloat16),
        cost_estimate=pl.CostEstimate(flops=8 * 2 * size**3, bytes_accessed=5 * 2**20, transcendentals=0),
        name="grams_%d" % relative_core,
    )(where, gradients)


def unfold(source, whole):
    whole[0:128, :] = source(0, 128, 0, 512)
    whole[128:256, 128:512] = source(128, 256, 128, 512)
    whole[384:512, 384:512] = source(128, 256, 0, 128)
    whole[256:320, 256:512] = source(256, 320, 0, 256)
    whole[320:384, 256:512] = source(256, 320, 256, 512)
    for i in range(4):
        for j in range(i + 1, 4):
            whole[j * 128 : j * 128 + 128, i * 128 : i * 128 + 128] = whole[
                i * 128 : i * 128 + 128, j * 128 : j * 128 + 128
            ].T


def newton_kernel(where_ref, own_ref, core_ref, far_ref, *rest):
    outs, whole = rest[:4], rest[4]
    size = whole.shape[0]

    def source(r0, r1, c0, c1):
        return (
            own_ref[0, r0:r1, c0:c1].astype(jnp.float32)
            + core_ref[0, r0:r1, c0:c1].astype(jnp.float32)
            + far_ref[0, r0:r1, c0:c1].astype(jnp.float32)
        ) * 0.25

    unfold(source, whole)
    identity = (iota2((size, size), 0) == iota2((size, size), 1)).astype(jnp.float32)
    statistic = whole[...]
    diagonal = jnp.sum(jnp.sum(statistic * identity, axis=0, keepdims=True), axis=1, keepdims=True) / size
    damped = statistic + 0.1 * diagonal * identity
    square = jnp.sum(jnp.sum(damped * damped, axis=0, keepdims=True), axis=1, keepdims=True) / (size * size)
    norm_scale = size * jnp.sqrt(square + 1e-06)
    root_scale = 1.0 / jnp.sqrt(jnp.sqrt(norm_scale))
    first = damped * (1.0 / norm_scale)

    def advance(matrix):
        part = matmul(matrix, matrix) * 0.0625 - 0.625 * matrix
        half = 1.5625 * matrix + matmul(part, matrix)
        return 1.5625 * half + matmul(part, half)

    second = advance(first)
    product = matmul(first, second) * 0.0625 - 0.3125 * (first + second)
    third = advance(second)
    rest_part = 1.25 * product - 0.390625 * third - 0.25 * matmul(product, third)
    whole[...] = rest_part * root_scale
    centre = root_scale * 1.953125
    high = centre.astype(jnp.bfloat16).astype(jnp.float32)
    low = centre - high
    for relative in range(4):
        target = where_ref[0] ^ relative
        rows = pl.multiple_of(target * 128, 128)
        outs[relative][0] = whole[pl.ds(rows, 128), :].astype(jnp.bfloat16)
        last = whole[pl.ds(rows + 112, 16), pl.ds(rows, 128)]
        row, lane = iota2((16, 128), 0), iota2((16, 128), 1)
        last = jnp.where((row == 15) & (lane == 0), high, last)
        last = jnp.where((row == 15) & (lane == 1), low, last)
        outs[relative][0, 112:128, pl.ds(rows, 128)] = last.astype(jnp.bfloat16)


def newton(where, own, core, far, chunk):
    size = own.shape[-1]
    folded = own.shape[-2]
    flat = lambda array: array.reshape(-1, folded, size)
    spec = lambda offset: pl.BlockSpec((1, folded, size), lambda step, where_ref: (offset + step, 0, 0))
    return pl.pallas_call(
        newton_kernel,
        grid_spec=pltpu.PrefetchScalarGridSpec(
            num_scalar_prefetch=1,
            grid=(2,),
            in_specs=[spec(4 + chunk * 2), spec(4 + chunk * 2), spec(0)],
            out_specs=[pl.BlockSpec((1, 128, size), lambda step, where_ref: (step, 0, 0))] * 4,
            scratch_shapes=[pltpu.VMEM((size, size), jnp.float32)],
        ),
        out_shape=[jax.ShapeDtypeStruct((2, 128, size), jnp.bfloat16)] * 4,
        cost_estimate=pl.CostEstimate(flops=16 * 2 * size**3, bytes_accessed=4 * 2**20, transcendentals=0),
        name="newton_%d" % chunk,
    )(where, flat(own), flat(core), flat(far))


def opened(tile):
    row, lane = iota2((128, 128), 0), iota2((128, 128), 1)
    line = iota2((1, 128), 1)
    last = tile[127:128, :]
    pick = lambda values, mask: jnp.sum(jnp.where(mask, values, 0.0), axis=1, keepdims=True)
    centre = pick(last, line < 2)
    first_value = pick(tile[0:1, :], line == 127)
    second_value = pick(tile[1:2, :], line == 127)
    tile = jnp.where((row == 127) & (lane == 0), first_value, tile)
    tile = jnp.where((row == 127) & (lane == 1), second_value, tile)
    return tile + jnp.where(row == lane, centre, 0.0)


def locate(stat, device):
    return (stat // 4) ^ device, (stat % 4) // 2, stat % 2


def gather_rows(where, refs, held):
    for chunk in range(2):
        for relative in range(4):
            for place in range(2):
                target = (where ^ relative) * 4 + chunk * 2 + place
                held[target] = refs[chunk * 4 + relative][place]


def slab_kernel(where_ref, *rest):
    refs, out_ref = rest[:8], rest[8]
    device = where_ref[0]
    columns = pl.multiple_of(device * 128, 128)
    for chunk in range(2):
        for relative in range(4):
            base = (device ^ relative) * 4 + chunk * 2

            def body(place, carry):
                value = refs[chunk * 4 + relative][place].astype(jnp.float32)
                out_ref[base + place] = value
                tile = refs[chunk * 4 + relative][place, :, pl.ds(columns, 128)].astype(jnp.float32)
                out_ref[base + place, :, pl.ds(columns, 128)] = opened(tile)
                return carry

            lax.fori_loop(0, 2, body, 0)


def slab_rows(where, pieces, stats):
    size = pieces[0].shape[-1]
    return pl.pallas_call(
        slab_kernel,
        in_specs=[pl.BlockSpec(memory_space=pltpu.SMEM)] + [pl.BlockSpec(memory_space=pltpu.VMEM)] * 8,
        out_specs=pl.BlockSpec(memory_space=pltpu.VMEM),
        out_shape=jax.ShapeDtypeStruct((stats, 128, size), jnp.float32),
        cost_estimate=pl.CostEstimate(flops=2**22, bytes_accessed=6 * 2**20, transcendentals=0),
        name="slab_rows",
    )(where, *pieces)


def send_kernel(where_ref, index_ref, valid_ref, *rest):
    refs, out_ref, held, tiles = rest[:8], rest[8], rest[9], rest[10]
    device = where_ref[0]
    gather_rows(device, refs, held)
    own = pl.multiple_of(device * 128, 128)
    after = pl.multiple_of(((device + 1) % 4) * 128, 128)
    across = pl.multiple_of((device ^ 2) * 128, 128)

    def body(place, carry):
        @pl.when(valid_ref[place] > 0)
        def _():
            stat = index_ref[place]
            for part in range(PARTS - 1):
                rows = slice(part * 32, part * 32 + 32)
                out_ref[part, place, :, 0:128] = held[stat, rows, pl.ds(own, 128)]
                out_ref[part, place, :, 128:256] = held[stat, rows, pl.ds(after, 128)]
            tile = held[stat, :, pl.ds(across, 128)].astype(jnp.float32)
            half = jnp.where(device < 2, tile[0:64, :], tile.T[64:128, :]).astype(jnp.bfloat16)
            out_ref[PARTS - 1, place, :, 0:128] = half[0:32, :]
            out_ref[PARTS - 1, place, :, 128:256] = half[32:64, :]

        @pl.when(valid_ref[place] == 0)
        def _():
            for part in range(PARTS):
                out_ref[part, place] = jnp.zeros(out_ref.shape[2:], out_ref.dtype)

        return carry

    lax.fori_loop(0, out_ref.shape[1], body, 0)


def send_rows(where, index, valid, pieces, stats):
    size = pieces[0].shape[-1]
    places = index.shape[0]
    smem = pl.BlockSpec(memory_space=pltpu.SMEM)
    return pl.pallas_call(
        send_kernel,
        in_specs=[smem] * 3 + [pl.BlockSpec(memory_space=pltpu.VMEM)] * 8,
        out_specs=pl.BlockSpec(memory_space=pltpu.VMEM),
        out_shape=jax.ShapeDtypeStruct((PARTS, places, 32, 256), jnp.bfloat16),
        scratch_shapes=[
            pltpu.VMEM((stats, 128, size), jnp.bfloat16),
            pltpu.VMEM((128, 128), jnp.float32),
        ],
        cost_estimate=pl.CostEstimate(flops=2**22, bytes_accessed=4 * 2**20, transcendentals=0),
        name="send_rows",
    )(where, index, valid, *pieces)


def route_kernel(pair_count, model_count, index_ref, valid_ref, sent_ref, out_ref, *scratch):
    held, slots = scratch[:PARTS], scratch[PARTS : 2 * PARTS]
    model_send, model_recv, data_send, data_recv = scratch[2 * PARTS :]
    me, device = lax.axis_index("mp"), lax.axis_index("dp")
    share = slots[0].shape[0] // 4
    barrier = pltpu.get_barrier_semaphore()
    for hop in range(1, model_count):
        pl.semaphore_signal(
            barrier, inc=1, device_id={"mp": lax.rem(me + hop, model_count)}, device_id_type=MESH
        )
    for relative in range(1, 4):
        pl.semaphore_signal(barrier, inc=1, device_id={"dp": device ^ relative}, device_id_type=MESH)
    pl.semaphore_wait(barrier, model_count + 2)

    own = pl.ds(me * pair_count, pair_count)
    to_owners = []
    for part in range(PARTS):
        for hop in range(1, model_count):
            owner = lax.rem(me + hop, model_count)
            copy = pltpu.make_async_remote_copy(
                src_ref=sent_ref.at[part, pl.ds(owner * pair_count, pair_count)],
                dst_ref=held[part].at[own],
                send_sem=model_send.at[part, hop - 1],
                recv_sem=model_recv.at[part, hop - 1],
                device_id={"mp": owner},
                device_id_type=MESH,
            )
            copy.start()
            to_owners.append(copy)
    for part in range(PARTS):
        held[part][own] = sent_ref[part, own]

    to_slots = []
    for part in range(PARTS):
        for hop in range(1, model_count):
            to_owners[part * (model_count - 1) + hop - 1].wait_recv()

        def place(slot, carry, part=part):
            value = held[part][index_ref[slot]]
            slots[part][slot] = jnp.where(valid_ref[slot] > 0, value, jnp.zeros_like(value))
            return carry

        lax.fori_loop(0, slots[part].shape[0], place, 0)
        for relative in (3, 2, 1):
            target = device ^ relative
            copy = pltpu.make_async_remote_copy(
                src_ref=slots[part].at[pl.ds(target * share, share)],
                dst_ref=out_ref.at[part, device],
                send_sem=data_send.at[part, relative - 1],
                recv_sem=data_recv.at[part, relative - 1],
                device_id={"dp": target},
                device_id_type=MESH,
            )
            copy.start()
            to_slots.append(copy)
        out_ref[part, device] = slots[part][pl.ds(device * share, share)]
    for copy in to_owners:
        copy.wait_send()
    for copy in to_slots:
        copy.wait()


def route(index, valid, sent, pair_count):
    model_count = lax.axis_size("mp")
    places = sent.shape[1]
    slots = index.shape[0]
    smem = pl.BlockSpec(memory_space=pltpu.SMEM)
    vmem = pl.BlockSpec(memory_space=pltpu.VMEM)
    return pl.pallas_call(
        functools.partial(route_kernel, pair_count, model_count),
        in_specs=[smem, smem, vmem],
        out_specs=vmem,
        out_shape=jax.ShapeDtypeStruct((PARTS, 4, slots // 4, 32, 256), jnp.bfloat16),
        scratch_shapes=[pltpu.VMEM((places, 32, 256), jnp.bfloat16)] * PARTS
        + [pltpu.VMEM((slots, 32, 256), jnp.bfloat16)] * PARTS
        + [pltpu.SemaphoreType.DMA((PARTS, model_count - 1))] * 2
        + [pltpu.SemaphoreType.DMA((PARTS, 3))] * 2,
        compiler_params=pltpu.CompilerParams(collective_id=0, has_side_effects=True),
        cost_estimate=pl.CostEstimate(flops=2**20, bytes_accessed=4 * 2**20, transcendentals=0),
        name="route",
    )(index, valid, sent)


def stack_kernel(piece_ref, out_ref):
    tile_at = lambda i: slice(i * 128, i * 128 + 128)

    def rows(i, lanes):
        parts = [piece_ref[part, i, 0, :, lanes].astype(jnp.float32) for part in range(PARTS - 1)]
        return jnp.concatenate(parts, axis=0)

    for i in range(4):
        out_ref[0, tile_at(i), tile_at(i)] = opened(rows(i, slice(0, 128)))
        j = (i + 1) % 4
        tile = rows(i, slice(128, 256))
        out_ref[0, tile_at(i), tile_at(j)] = tile
        out_ref[0, tile_at(j), tile_at(i)] = tile.T
    for i in range(2):
        parts = []
        for source in (i, i + 2):
            parts += [piece_ref[PARTS - 1, source, 0, :, 0:128], piece_ref[PARTS - 1, source, 0, :, 128:256]]
        tile = jnp.concatenate([part.astype(jnp.float32) for part in parts], axis=0)
        out_ref[0, tile_at(i), tile_at(i + 2)] = tile
        out_ref[0, tile_at(i + 2), tile_at(i)] = tile.T


def stack_rows(pieces, size):
    slots = pieces.shape[2]
    return pl.pallas_call(
        stack_kernel,
        grid=(slots,),
        in_specs=[pl.BlockSpec((PARTS, 4, 1, 32, 256), lambda slot: (0, 0, slot, 0, 0))],
        out_specs=pl.BlockSpec((1, size, size), lambda slot: (slot, 0, 0)),
        out_shape=jax.ShapeDtypeStruct((slots, size, size), jnp.float32),
        cost_estimate=pl.CostEstimate(flops=2**22, bytes_accessed=8 * 2**20, transcendentals=0),
        name="stack_rows",
    )(pieces)


def exchange(array, relative):
    return lax.ppermute(array, "dp", [(i, i ^ relative) for i in range(4)])


def on_quad(gradients, owner_table):
    model_count = lax.axis_size("mp")
    model_index = lax.axis_index("mp")
    device = lax.axis_index("dp")
    where = device.astype(jnp.int32).reshape(1)
    size = gradients.shape[2]
    per_slab = 2 * (gradients.shape[1] // size)
    pair_count = (CAP + model_count - 1) // model_count
    targets, stack_index, stack_valid, _ = make_plan(
        owner_table, model_index, model_count, per_slab, pair_count
    )
    places = jnp.arange(model_count * pair_count, dtype=jnp.int32)
    send_match = (places[:, None] == targets[None, :]).astype(jnp.int32)
    send_index = jnp.sum(send_match * jnp.arange(per_slab, dtype=jnp.int32)[None, :], axis=1)
    send_valid = jnp.sum(send_match, axis=1)

    received = exchange(grams(where, gradients, 1), 1)
    own = grams(where, gradients, 0)
    pieces = []
    for chunk in range(2):
        summed = (own[chunk].astype(jnp.float32) + received[chunk].astype(jnp.float32)).astype(jnp.bfloat16)
        far = exchange(summed, 2)
        roots = newton(where, own, received, far, chunk)
        pieces += [roots[0]] + [exchange(roots[relative], relative) for relative in (1, 2, 3)]
    sent = send_rows(where, send_index, send_valid, pieces, per_slab)
    slab = slab_rows(where, pieces, per_slab)
    stacks = stack_rows(route(stack_index, stack_valid, sent, pair_count), size)
    return (stacks[None], slab)


def solution(mesh):
    placed = (P("dp", None, "mp"), P())

    def body(gradients, owner_table):
        size = gradients.shape[2]
        row_blocks = gradients.shape[1] // size
        if lax.axis_size("dp") == 4 and size == 512 and row_blocks == 8:
            return on_quad(gradients, owner_table)
        return on_device(gradients, owner_table)

    return jax.shard_map(
        body,
        mesh=mesh,
        in_specs=placed,
        out_specs=(P("mp", "dp", None, None), P(None, "dp", "mp")),
        check_vma=False,
    )
```

```python
import functools

import jax
import jax.numpy as jnp
from jax import lax
from jax.experimental import pallas as pl
from jax.experimental.pallas import tpu as pltpu
from jax.sharding import PartitionSpec as P

ITERS = 3
CAP = 24
PARTS = 5
MESH = pl.DeviceIdType.MESH


def batched(first, second):
    return jnp.einsum("kab,kbc->kac", first, second, precision=lax.Precision.HIGHEST)


def newton_roots(statistics, iterations):
    matrix_size = statistics.shape[-1]
    identity = jnp.eye(matrix_size, dtype=jnp.float32)
    diagonal_mean = jnp.mean(jnp.diagonal(statistics, axis1=1, axis2=2), axis=1)
    damped = statistics + 0.1 * diagonal_mean[:, None, None] * identity[None]
    mean_square = jnp.mean(damped * damped, axis=(1, 2))
    norm_scale = matrix_size * jnp.sqrt(mean_square + 1e-06)
    matrix = damped / norm_scale[:, None, None]
    root_scale = norm_scale ** (-0.25)
    current = matrix
    for iteration in range(iterations):
        factor = (5.0 * identity - matrix) * 0.25
        if iteration == 0:
            current = factor * root_scale[:, None, None]
        else:
            current = batched(current, factor)
        if iteration + 1 < iterations:
            square = batched(factor, factor)
            matrix = batched(square, batched(square, matrix))
    return current


def pick_rows(source, match_table):
    labels = jnp.arange(match_table.shape[1], dtype=jnp.int32)
    pick_index = jnp.sum(match_table * labels[None, :], axis=1)
    is_valid = jnp.sum(match_table, axis=1).astype(jnp.float32)
    return jnp.take(source, pick_index, axis=0) * is_valid[:, None, None]


def make_plan(owner_table, model_index, model_count, per_slab, pair_count):
    stat_count = owner_table.shape[0]
    owner_ids = jnp.arange(model_count, dtype=jnp.int32)
    onehot = (owner_table[:, None] == owner_ids[None, :]).astype(jnp.int32)
    slot_number = jnp.sum((jnp.cumsum(onehot, axis=0) - onehot) * onehot, axis=1)
    owner_grid = onehot.reshape(model_count, per_slab, model_count)
    pair_rank = jnp.sum((jnp.cumsum(owner_grid, axis=1) - owner_grid) * owner_grid, axis=2).reshape(
        stat_count
    )
    stat_ids = jnp.arange(stat_count, dtype=jnp.int32)
    position = stat_ids // per_slab * pair_count + pair_rank
    owner_loads = jnp.sum(onehot, axis=0)
    first_stat = model_index * per_slab
    targets = lax.dynamic_slice_in_dim(owner_table * pair_count + pair_rank, first_stat, per_slab)
    slot_ids = jnp.arange(CAP, dtype=jnp.int32)
    slot_match = (
        (owner_table[None, :] == model_index) & (slot_number[None, :] == slot_ids[:, None])
    ).astype(jnp.int32)
    stack_index = jnp.sum(slot_match * position[None, :], axis=1)
    stack_valid = jnp.sum(slot_match, axis=1)
    return (targets, stack_index, stack_valid, owner_loads)


def to_owner(pieces, route_plan, model_count, pair_count):
    targets, stack_index, stack_valid, owner_loads = route_plan
    places = jnp.arange(model_count * pair_count, dtype=jnp.int32)
    send_match = (places[:, None] == targets[None, :]).astype(jnp.int32)
    incoming = lax.all_to_all(
        pick_rows(pieces, send_match), "mp", split_axis=0, concat_axis=0, tiled=True
    )
    slot_match = (stack_index[:, None] == places[None, :]).astype(jnp.int32) * stack_valid[:, None]
    slot_stack = pick_rows(incoming, slot_match)
    return lax.all_to_all(slot_stack, "dp", split_axis=0, concat_axis=1, tiled=True)


def row_sums(rounded, data_count):
    return lax.psum_scatter(
        rounded.astype(jnp.bfloat16), "dp", scatter_dimension=1, tiled=True
    ).astype(jnp.float32) * (1.0 / data_count)


def on_device(gradients, owner_table):
    data_count = lax.axis_size("dp")
    model_count = lax.axis_size("mp")
    model_index = lax.axis_index("mp")
    block_size = gradients.shape[2]
    row_blocks = gradients.shape[1] // block_size
    per_slab = 2 * row_blocks
    pair_count = (CAP + model_count - 1) // model_count
    local_blocks = gradients[0].reshape(row_blocks, block_size, block_size)
    left_gram = jnp.einsum(
        "rab,rcb->rac", local_blocks, local_blocks, preferred_element_type=jnp.float32
    )
    right_gram = jnp.einsum(
        "rab,rac->rbc", local_blocks, local_blocks, preferred_element_type=jnp.float32
    )
    partial_value = jnp.stack([left_gram, right_gram], axis=1).reshape(
        per_slab, block_size, block_size
    )
    rounded = lax.optimization_barrier(partial_value.astype(jnp.bfloat16)).astype(jnp.float32)
    route_plan = make_plan(owner_table, model_index, model_count, per_slab, pair_count)
    stat_sums = row_sums(rounded, data_count)
    whole_stats = lax.all_to_all(stat_sums, "dp", split_axis=0, concat_axis=1, tiled=True)
    home_roots = newton_roots(whole_stats, ITERS)
    slab_roots = lax.all_to_all(home_roots, "dp", split_axis=1, concat_axis=0, tiled=True)
    root_stacks = to_owner(slab_roots, route_plan, model_count, pair_count)
    return (root_stacks[None], slab_roots)


def iota2(shape, axis):
    return lax.broadcasted_iota(jnp.int32, shape, axis)


def matmul(first, second):
    return jnp.dot(
        first.astype(jnp.bfloat16), second.astype(jnp.bfloat16), preferred_element_type=jnp.float32
    )


def fold_upper(store, full):
    store(0, 128, 0, 512, full[0:128, :])
    store(128, 256, 128, 512, full[128:256, 128:512])
    store(128, 256, 0, 128, full[384:512, 384:512])
    store(256, 320, 0, 256, full[256:320, 256:512])
    store(256, 320, 256, 512, full[320:384, 256:512])


def gram_kernel(where_ref, grad_ref, out_ref):
    block = grad_ref[0]
    for kind in range(2):
        flipped = block.T
        full = jnp.dot(block, flipped, preferred_element_type=jnp.float32) if kind == 0 else jnp.dot(
            flipped, block, preferred_element_type=jnp.float32
        )
        full = full.astype(jnp.bfloat16)

        def store(r0, r1, c0, c1, value, kind=kind):
            out_ref[0, kind, r0:r1, c0:c1] = value

        fold_upper(store, full)


def grams(where, gradients, relative_core):
    size = gradients.shape[2]

    def grad_map(step, where_ref):
        target = where_ref[0] ^ relative_core ^ ((1 - step // 2) * 2)
        return (0, target * 2 + step % 2, 0)

    return pl.pallas_call(
        gram_kernel,
        grid_spec=pltpu.PrefetchScalarGridSpec(
            num_scalar_prefetch=1,
            grid=(4,),
            in_specs=[pl.BlockSpec((1, size, size), grad_map)],
            out_specs=pl.BlockSpec((1, 2, 320, size), lambda step, where_ref: (step, 0, 0, 0)),
        ),
        out_shape=jax.ShapeDtypeStruct((4, 2, 320, size), jnp.bfloat16),
        cost_estimate=pl.CostEstimate(flops=8 * 2 * size**3, bytes_accessed=5 * 2**20, transcendentals=0),
        name="grams_%d" % relative_core,
    )(where, gradients)


def unfold(source, whole):
    whole[0:128, :] = source(0, 128, 0, 512)
    whole[128:256, 128:512] = source(128, 256, 128, 512)
    whole[384:512, 384:512] = source(128, 256, 0, 128)
    whole[256:320, 256:512] = source(256, 320, 0, 256)
    whole[320:384, 256:512] = source(256, 320, 256, 512)
    for i in range(4):
        for j in range(i + 1, 4):
            whole[j * 128 : j * 128 + 128, i * 128 : i * 128 + 128] = whole[
                i * 128 : i * 128 + 128, j * 128 : j * 128 + 128
            ].T


def newton_kernel(where_ref, own_ref, core_ref, far_ref, *rest):
    outs, whole = rest[:4], rest[4]
    size = whole.shape[0]

    def source(r0, r1, c0, c1):
        return (
            own_ref[0, r0:r1, c0:c1].astype(jnp.float32)
            + core_ref[0, r0:r1, c0:c1].astype(jnp.float32)
            + far_ref[0, r0:r1, c0:c1].astype(jnp.float32)
        ) * 0.25

    unfold(source, whole)
    identity = (iota2((size, size), 0) == iota2((size, size), 1)).astype(jnp.float32)
    statistic = whole[...]
    diagonal = jnp.sum(jnp.sum(statistic * identity, axis=0, keepdims=True), axis=1, keepdims=True) / size
    damped = statistic + 0.1 * diagonal * identity
    square = jnp.sum(jnp.sum(damped * damped, axis=0, keepdims=True), axis=1, keepdims=True) / (size * size)
    norm_scale = size * jnp.sqrt(square + 1e-06)
    root_scale = 1.0 / jnp.sqrt(jnp.sqrt(norm_scale))
    first = damped * (1.0 / norm_scale)

    def advance(matrix):
        part = matmul(matrix, matrix) * 0.0625 - 0.625 * matrix
        half = 1.5625 * matrix + matmul(part, matrix)
        return 1.5625 * half + matmul(part, half)

    second = advance(first)
    product = matmul(first, second) * 0.0625 - 0.3125 * (first + second)
    third = advance(second)
    rest_part = 1.25 * product - 0.390625 * third - 0.25 * matmul(product, third)
    whole[...] = rest_part * root_scale
    centre = root_scale * 1.953125
    high = centre.astype(jnp.bfloat16).astype(jnp.float32)
    low = centre - high
    for relative in range(4):
        target = where_ref[0] ^ relative
        rows = pl.multiple_of(target * 128, 128)
        outs[relative][0] = whole[pl.ds(rows, 128), :].astype(jnp.bfloat16)
        last = whole[pl.ds(rows + 112, 16), pl.ds(rows, 128)]
        row, lane = iota2((16, 128), 0), iota2((16, 128), 1)
        last = jnp.where((row == 15) & (lane == 0), high, last)
        last = jnp.where((row == 15) & (lane == 1), low, last)
        outs[relative][0, 112:128, pl.ds(rows, 128)] = last.astype(jnp.bfloat16)


def newton(where, own, core, far, chunk):
    size = own.shape[-1]
    folded = own.shape[-2]
    flat = lambda array: array.reshape(-1, folded, size)
    spec = lambda offset: pl.BlockSpec((1, folded, size), lambda step, where_ref: (offset + step, 0, 0))
    return pl.pallas_call(
        newton_kernel,
        grid_spec=pltpu.PrefetchScalarGridSpec(
            num_scalar_prefetch=1,
            grid=(2,),
            in_specs=[spec(4 + chunk * 2), spec(4 + chunk * 2), spec(0)],
            out_specs=[pl.BlockSpec((1, 128, size), lambda step, where_ref: (step, 0, 0))] * 4,
            scratch_shapes=[pltpu.VMEM((size, size), jnp.float32)],
        ),
        out_shape=[jax.ShapeDtypeStruct((2, 128, size), jnp.bfloat16)] * 4,
        cost_estimate=pl.CostEstimate(flops=16 * 2 * size**3, bytes_accessed=4 * 2**20, transcendentals=0),
        name="newton_%d" % chunk,
    )(where, flat(own), flat(core), flat(far))


def opened(tile):
    row, lane = iota2((128, 128), 0), iota2((128, 128), 1)
    line = iota2((1, 128), 1)
    last = tile[127:128, :]
    pick = lambda values, mask: jnp.sum(jnp.where(mask, values, 0.0), axis=1, keepdims=True)
    centre = pick(last, line < 2)
    first_value = pick(tile[0:1, :], line == 127)
    second_value = pick(tile[1:2, :], line == 127)
    tile = jnp.where((row == 127) & (lane == 0), first_value, tile)
    tile = jnp.where((row == 127) & (lane == 1), second_value, tile)
    return tile + jnp.where(row == lane, centre, 0.0)


def locate(stat, device):
    return (stat // 4) ^ device, (stat % 4) // 2, stat % 2


def gather_rows(where, refs, held):
    for chunk in range(2):
        for relative in range(4):
            for place in range(2):
                target = (where ^ relative) * 4 + chunk * 2 + place
                held[target] = refs[chunk * 4 + relative][place]


def slab_kernel(where_ref, *rest):
    refs, out_ref = rest[:8], rest[8]
    columns = pl.multiple_of(where_ref[0] * 128, 128)
    for source in range(8):

        @pl.when(pl.program_id(0) == source)
        def _(source=source):
            for place in range(2):
                out_ref[place] = refs[source][place].astype(jnp.float32)
                tile = refs[source][place, :, pl.ds(columns, 128)].astype(jnp.float32)
                out_ref[place, :, pl.ds(columns, 128)] = opened(tile)


def slab_rows(where, pieces, stats):
    size = pieces[0].shape[-1]
    return pl.pallas_call(
        slab_kernel,
        grid_spec=pltpu.PrefetchScalarGridSpec(
            num_scalar_prefetch=1,
            grid=(8,),
            in_specs=[pl.BlockSpec((2, 128, size), lambda step, where_ref: (0, 0, 0))] * 8,
            out_specs=pl.BlockSpec(
                (2, 128, size),
                lambda step, where_ref: ((where_ref[0] ^ (step % 4)) * 2 + step // 4, 0, 0),
            ),
        ),
        out_shape=jax.ShapeDtypeStruct((stats, 128, size), jnp.float32),
        cost_estimate=pl.CostEstimate(flops=2**22, bytes_accessed=6 * 2**20, transcendentals=0),
        name="slab_rows",
    )(where, *pieces)


def send_kernel(where_ref, index_ref, valid_ref, *rest):
    refs, out_ref, held, tiles = rest[:8], rest[8], rest[9], rest[10]
    device = where_ref[0]
    gather_rows(device, refs, held)
    own = pl.multiple_of(device * 128, 128)
    after = pl.multiple_of(((device + 1) % 4) * 128, 128)
    across = pl.multiple_of((device ^ 2) * 128, 128)

    def body(place, carry):
        @pl.when(valid_ref[place] > 0)
        def _():
            stat = index_ref[place]
            for part in range(PARTS - 1):
                rows = slice(part * 32, part * 32 + 32)
                out_ref[part, place, :, 0:128] = held[stat, rows, pl.ds(own, 128)]
                out_ref[part, place, :, 128:256] = held[stat, rows, pl.ds(after, 128)]
            tile = held[stat, :, pl.ds(across, 128)].astype(jnp.float32)
            half = jnp.where(device < 2, tile[0:64, :], tile.T[64:128, :]).astype(jnp.bfloat16)
            out_ref[PARTS - 1, place, :, 0:128] = half[0:32, :]
            out_ref[PARTS - 1, place, :, 128:256] = half[32:64, :]

        @pl.when(valid_ref[place] == 0)
        def _():
            for part in range(PARTS):
                out_ref[part, place] = jnp.zeros(out_ref.shape[2:], out_ref.dtype)

        return carry

    lax.fori_loop(0, out_ref.shape[1], body, 0)


def send_rows(where, index, valid, pieces, stats):
    size = pieces[0].shape[-1]
    places = index.shape[0]
    smem = pl.BlockSpec(memory_space=pltpu.SMEM)
    return pl.pallas_call(
        send_kernel,
        in_specs=[smem] * 3 + [pl.BlockSpec(memory_space=pltpu.VMEM)] * 8,
        out_specs=pl.BlockSpec(memory_space=pltpu.VMEM),
        out_shape=jax.ShapeDtypeStruct((PARTS, places, 32, 256), jnp.bfloat16),
        scratch_shapes=[
            pltpu.VMEM((stats, 128, size), jnp.bfloat16),
            pltpu.VMEM((128, 128), jnp.float32),
        ],
        cost_estimate=pl.CostEstimate(flops=2**22, bytes_accessed=4 * 2**20, transcendentals=0),
        name="send_rows",
    )(where, index, valid, *pieces)


def route_kernel(pair_count, model_count, index_ref, valid_ref, sent_ref, out_ref, *scratch):
    held, slots = scratch[:PARTS], scratch[PARTS : 2 * PARTS]
    model_send, model_recv, data_send, data_recv = scratch[2 * PARTS :]
    me, device = lax.axis_index("mp"), lax.axis_index("dp")
    share = slots[0].shape[0] // 4
    barrier = pltpu.get_barrier_semaphore()
    for hop in range(1, model_count):
        pl.semaphore_signal(
            barrier, inc=1, device_id={"mp": lax.rem(me + hop, model_count)}, device_id_type=MESH
        )
    for relative in range(1, 4):
        pl.semaphore_signal(barrier, inc=1, device_id={"dp": device ^ relative}, device_id_type=MESH)
    pl.semaphore_wait(barrier, model_count + 2)

    own = pl.ds(me * pair_count, pair_count)
    to_owners = []
    for part in range(PARTS):
        for hop in range(1, model_count):
            owner = lax.rem(me + hop, model_count)
            copy = pltpu.make_async_remote_copy(
                src_ref=sent_ref.at[part, pl.ds(owner * pair_count, pair_count)],
                dst_ref=held[part].at[own],
                send_sem=model_send.at[part, hop - 1],
                recv_sem=model_recv.at[part, hop - 1],
                device_id={"mp": owner},
                device_id_type=MESH,
            )
            copy.start()
            to_owners.append(copy)
    for part in range(PARTS):
        held[part][own] = sent_ref[part, own]

    to_slots = []
    for part in range(PARTS):
        for hop in range(1, model_count):
            to_owners[part * (model_count - 1) + hop - 1].wait_recv()

        def place(slot, carry, part=part):
            value = held[part][index_ref[slot]]
            slots[part][slot] = jnp.where(valid_ref[slot] > 0, value, jnp.zeros_like(value))
            return carry

        lax.fori_loop(0, slots[part].shape[0], place, 0)
        for relative in (3, 2, 1):
            target = device ^ relative
            copy = pltpu.make_async_remote_copy(
                src_ref=slots[part].at[pl.ds(target * share, share)],
                dst_ref=out_ref.at[part, device],
                send_sem=data_send.at[part, relative - 1],
                recv_sem=data_recv.at[part, relative - 1],
                device_id={"dp": target},
                device_id_type=MESH,
            )
            copy.start()
            to_slots.append(copy)
        out_ref[part, device] = slots[part][pl.ds(device * share, share)]
    for copy in to_owners:
        copy.wait_send()
    for copy in to_slots:
        copy.wait()


def route(index, valid, sent, pair_count):
    model_count = lax.axis_size("mp")
    places = sent.shape[1]
    slots = index.shape[0]
    smem = pl.BlockSpec(memory_space=pltpu.SMEM)
    vmem = pl.BlockSpec(memory_space=pltpu.VMEM)
    return pl.pallas_call(
        functools.partial(route_kernel, pair_count, model_count),
        in_specs=[smem, smem, vmem],
        out_specs=vmem,
        out_shape=jax.ShapeDtypeStruct((PARTS, 4, slots // 4, 32, 256), jnp.bfloat16),
        scratch_shapes=[pltpu.VMEM((places, 32, 256), jnp.bfloat16)] * PARTS
        + [pltpu.VMEM((slots, 32, 256), jnp.bfloat16)] * PARTS
        + [pltpu.SemaphoreType.DMA((PARTS, model_count - 1))] * 2
        + [pltpu.SemaphoreType.DMA((PARTS, 3))] * 2,
        compiler_params=pltpu.CompilerParams(collective_id=0, has_side_effects=True),
        cost_estimate=pl.CostEstimate(flops=2**20, bytes_accessed=4 * 2**20, transcendentals=0),
        name="route",
    )(index, valid, sent)


def stack_kernel(piece_ref, out_ref):
    tile_at = lambda i: slice(i * 128, i * 128 + 128)

    def rows(i, lanes):
        parts = [piece_ref[part, i, 0, :, lanes].astype(jnp.float32) for part in range(PARTS - 1)]
        return jnp.concatenate(parts, axis=0)

    for i in range(4):
        out_ref[0, tile_at(i), tile_at(i)] = opened(rows(i, slice(0, 128)))
        j = (i + 1) % 4
        tile = rows(i, slice(128, 256))
        out_ref[0, tile_at(i), tile_at(j)] = tile
        out_ref[0, tile_at(j), tile_at(i)] = tile.T
    for i in range(2):
        parts = []
        for source in (i, i + 2):
            parts += [piece_ref[PARTS - 1, source, 0, :, 0:128], piece_ref[PARTS - 1, source, 0, :, 128:256]]
        tile = jnp.concatenate([part.astype(jnp.float32) for part in parts], axis=0)
        out_ref[0, tile_at(i), tile_at(i + 2)] = tile
        out_ref[0, tile_at(i + 2), tile_at(i)] = tile.T


def stack_rows(pieces, size):
    slots = pieces.shape[2]
    return pl.pallas_call(
        stack_kernel,
        grid=(slots,),
        in_specs=[pl.BlockSpec((PARTS, 4, 1, 32, 256), lambda slot: (0, 0, slot, 0, 0))],
        out_specs=pl.BlockSpec((1, size, size), lambda slot: (slot, 0, 0)),
        out_shape=jax.ShapeDtypeStruct((slots, size, size), jnp.float32),
        cost_estimate=pl.CostEstimate(flops=2**22, bytes_accessed=8 * 2**20, transcendentals=0),
        name="stack_rows",
    )(pieces)


def exchange(array, relative):
    return lax.ppermute(array, "dp", [(i, i ^ relative) for i in range(4)])


def on_quad(gradients, owner_table):
    model_count = lax.axis_size("mp")
    model_index = lax.axis_index("mp")
    device = lax.axis_index("dp")
    where = device.astype(jnp.int32).reshape(1)
    size = gradients.shape[2]
    per_slab = 2 * (gradients.shape[1] // size)
    pair_count = (CAP + model_count - 1) // model_count
    targets, stack_index, stack_valid, _ = make_plan(
        owner_table, model_index, model_count, per_slab, pair_count
    )
    places = jnp.arange(model_count * pair_count, dtype=jnp.int32)
    send_match = (places[:, None] == targets[None, :]).astype(jnp.int32)
    send_index = jnp.sum(send_match * jnp.arange(per_slab, dtype=jnp.int32)[None, :], axis=1)
    send_valid = jnp.sum(send_match, axis=1)

    received = exchange(grams(where, gradients, 1), 1)
    own = grams(where, gradients, 0)
    pieces = []
    for chunk in range(2):
        summed = (own[chunk].astype(jnp.float32) + received[chunk].astype(jnp.float32)).astype(jnp.bfloat16)
        far = exchange(summed, 2)
        roots = newton(where, own, received, far, chunk)
        pieces += [roots[0]] + [exchange(roots[relative], relative) for relative in (1, 2, 3)]
    sent = send_rows(where, send_index, send_valid, pieces, per_slab)
    slab = slab_rows(where, pieces, per_slab)
    stacks = stack_rows(route(stack_index, stack_valid, sent, pair_count), size)
    return (stacks[None], slab)


def solution(mesh):
    placed = (P("dp", None, "mp"), P())

    def body(gradients, owner_table):
        size = gradients.shape[2]
        row_blocks = gradients.shape[1] // size
        if lax.axis_size("dp") == 4 and size == 512 and row_blocks == 8:
            return on_quad(gradients, owner_table)
        return on_device(gradients, owner_table)

    return jax.shard_map(
        body,
        mesh=mesh,
        in_specs=placed,
        out_specs=(P("mp", "dp", None, None), P(None, "dp", "mp")),
        check_vma=False,
    )
```
